32 devices in a mesh: head: 4 (over x, core), seq: 8 (over z, y).
Axes of the slice: x: 2, y: 2, z: 4, core: 2. Of those that a mesh axis runs over, the one named last changes fastest.
Arguments:
- query: float32 [4096, 2048], P(('seq', 'head')), may hold values from -8 to 8
- key_in: float32 [4096, 1024], P(('seq', 'head')), may hold values from -8 to 8
- value_in: float32 [4096, 1024], P(('seq', 'head')), may hold values from -6 to 6
- d_out: float32 [4096, 2048], P(('seq', 'head')), may hold values from -48 to 48
Outputs:
- grad_query: float32 [4096, 2048], P(('seq', 'head'))
- grad_key: float32 [4096, 1024], P(('seq', 'head'))
- grad_value: float32 [4096, 1024], P(('seq', 'head'))
The draws below stay inside these ranges and needn't reach their ends.
All inputs are finite; a program needn't handle non-finite values.
Results may differ from the reference program's by a relative error of at most 0.00045.
Values sent between devices are 32-bit elements; how exact they have to be, the bound alone decides.
No kernel may reach another device: no remote copies, remote signals or barrier semaphores. Data moves between devices by JAX's collectives and lax.ppermute only.
A program may use at most 64 MiB of HBM per device.

```python
import jax
import jax.numpy as jnp
from jax import lax

HD = 128
QHEADS = 16
KVHEADS = 8
TOK_DEV = 512
WINDOW = 1024
TOKENS = 4096
N_SEQ = 8


def draw_query(key, part):
    base = jax.random.normal(jax.random.fold_in(key, 11), (TOKENS, QHEADS * HD), jnp.float32)
    return jnp.clip(base, -8.0, 8.0)


def draw_key_in(key, part):
    base = jax.random.normal(jax.random.fold_in(key, 12), (TOKENS, KVHEADS * HD), jnp.float32)
    return jnp.clip(base, -8.0, 8.0)


def steps_of(rng, dims, cuts, least, high):
    level = 1.0
    for position, parts in cuts:
        draws = jax.random.uniform(jax.random.fold_in(jax.random.fold_in(rng, 6), position), (parts,), jnp.float32, least / len(cuts), high / len(cuts))
        level = level * jnp.repeat(jnp.exp(draws), dims[position] // parts).reshape((-1,) + (1,) * (len(dims) - 1 - position))
    return level


def centred(own_key, dims, spread, most, split=(), kind=jnp.bfloat16):
    result = jax.random.normal(own_key, dims, jnp.float32) * spread
    if len(split) > 0:
        result = steps_of(own_key, dims, split, -0.22, 0.18) * result
    return jnp.clip(result, min=-most, max=most).astype(kind)


def setup_inputs(seed: int = 0) -> dict:
    arg_keys = jax.random.split(jax.random.key(seed), 5)
    return {
        "query": draw_query(jax.random.fold_in(arg_keys[4], 71), 0),
        "key_in": draw_key_in(jax.random.fold_in(arg_keys[4], 71), 0),
        "value_in": centred(arg_keys[2], (TOKENS, KVHEADS * HD), 1.0, 6.0, ((0, 32),), jnp.float32),
        "d_out": centred(arg_keys[3], (TOKENS, QHEADS * HD), 8.0, 48.0, ((0, 32),), jnp.float32),
    }


score_scale = 168.0 ** -0.5
highest = lax.Precision.HIGHEST


def band_grads(query_block, key_block, value_block, grad_block, start, reach):
    shard_rows = query_block.shape[0]
    key_rows = key_block.shape[0]
    group_size = query_block.shape[1] // key_block.shape[1]
    query_heads = query_block.reshape(shard_rows, -1, group_size, HD)
    grad_heads = grad_block.reshape(shard_rows, -1, group_size, HD)
    key_heads = key_block.reshape(key_rows, -1, HD)
    value_heads = value_block.reshape(key_rows, -1, HD)
    scores = jnp.einsum("qkgd,pkd->kgqp", query_heads, key_heads, precision=highest) * score_scale
    query_index = start + jnp.arange(shard_rows, dtype=jnp.int32)[:, None]
    key_index = start - 2 * shard_rows + jnp.arange(key_rows, dtype=jnp.int32)[None, :]
    inside = (key_index <= query_index) & (key_index > query_index - reach) & (key_index >= 0)
    scores = jnp.where(inside, scores, -jnp.inf)
    highest_score = jnp.max(scores, axis=-1, keepdims=True)
    raised = jnp.exp(scores - highest_score)
    weights = raised / jnp.sum(raised, axis=-1, keepdims=True)
    output = jnp.einsum("kgqp,pkd->qkgd", weights, value_heads, precision=highest)
    row_dot = jnp.einsum("qkgd,qkgd->kgq", grad_heads, output, precision=highest)
    grad_weight = jnp.einsum("qkgd,pkd->kgqp", grad_heads, value_heads, precision=highest)
    grad_score = weights * (grad_weight - row_dot[..., None])
    grad_query = jnp.einsum("kgqp,pkd->qkgd", grad_score, key_heads, precision=highest) * score_scale
    grad_key = jnp.einsum("kgqp,qkgd->pkd", grad_score, query_heads, precision=highest) * score_scale
    grad_value = jnp.einsum("kgqp,qkgd->pkd", weights, grad_heads, precision=highest)
    return (grad_query.reshape(shard_rows, -1), grad_key.reshape(key_rows, -1), grad_value.reshape(key_rows, -1))


def reference(query, key_in, value_in, d_out):
    shard_rows = TOK_DEV
    front = jnp.zeros((2 * shard_rows, key_in.shape[1]), jnp.float32)
    key_padded = jnp.concatenate([front, key_in], axis=0)
    value_padded = jnp.concatenate([front, value_in], axis=0)

    def step(totals, block_id):
        key_total, value_total = totals
        start = block_id * shard_rows
        query_block = lax.dynamic_slice_in_dim(query, start, shard_rows, 0)
        grad_block = lax.dynamic_slice_in_dim(d_out, start, shard_rows, 0)
        key_block = lax.dynamic_slice_in_dim(key_padded, start, 3 * shard_rows, 0)
        value_block = lax.dynamic_slice_in_dim(value_padded, start, 3 * shard_rows, 0)
        grad_query, grad_key, grad_value = band_grads(query_block, key_block, value_block, grad_block, start, WINDOW)
        key_total = lax.dynamic_update_slice_in_dim(key_total, lax.dynamic_slice_in_dim(key_total, start, 3 * shard_rows, 0) + grad_key, start, 0)
        value_total = lax.dynamic_update_slice_in_dim(value_total, lax.dynamic_slice_in_dim(value_total, start, 3 * shard_rows, 0) + grad_value, start, 0)
        return (key_total, value_total), grad_query

    init = (jnp.zeros_like(key_padded), jnp.zeros_like(value_padded))
    (key_total, value_total), query_parts = lax.scan(step, init, jnp.arange(N_SEQ, dtype=jnp.int32))
    return (query_parts.reshape(TOKENS, -1), key_total[2 * shard_rows:], value_total[2 * shard_rows:])
```

```python
import functools
import math

import jax
import jax.numpy as jnp
from jax import lax
from jax.experimental import pallas as pl
from jax.experimental.pallas import tpu as pltpu
from jax.sharding import PartitionSpec as P

HD = 128
WINDOW = 1024
QT = 256
KC = 128

score_scale = 168.0 ** (-0.5)
LOG2E = 1.0 / math.log(2.0)
f32 = jnp.float32
bf16 = jnp.bfloat16
BIG = 3.0e38


def split(x):
    hi = x.astype(bf16)
    lo = (x - hi.astype(f32)).astype(bf16)
    return hi, lo


def dot(a, b):
    return jnp.dot(a, b, preferred_element_type=f32)


def fold8(x, op):
    rows, cols = x.shape
    return op(x.reshape(rows // 8, 8, cols), axis=0)


def attn_kernel(
    group, first_ref, qd_ref, own_ref, far_ref, dq_ref, down_ref, dfar_ref,
    kaug, vaug, kt, dkacc, dvacc, sref, pref, dpref, phi, plo, dshi, dslo,
):
    t = pl.program_id(0)
    tokens = own_ref.shape[0]
    span = tokens + QT
    far_tiles = tokens // QT

    @pl.when(t == 0)
    def _():
        for base, ref in ((0, far_ref), (tokens, own_ref)):
            for r in range(0, tokens, QT):
                k = ref[pl.ds(r, QT), :HD]
                v = ref[pl.ds(r, QT), HD:]
                hi, lo = split(k)
                kaug[pl.ds(base + r, QT), :HD] = hi
                kaug[pl.ds(base + r, QT), HD:] = lo
                vh, vl = split(v)
                vaug[pl.ds(base + r, QT), :HD] = vh
                vaug[pl.ds(base + r, QT), HD:] = vl
                th, tl = split(k.T)
                kt[:HD, pl.ds(base + r, QT)] = th
                kt[HD:, pl.ds(base + r, QT)] = tl
        dkacc[...] = jnp.zeros_like(dkacc)
        dvacc[...] = jnp.zeros_like(dvacc)

    a = pl.multiple_of(t * QT, QT)
    first = first_ref[0] == 1
    rows = lax.broadcasted_iota(jnp.int32, (KC, QT), 0)
    cols = lax.broadcasted_iota(jnp.int32, (KC, QT), 1)
    rhs_q = []
    rhs_o = []
    for h in range(group):
        q = qd_ref[:, h * HD:(h + 1) * HD] * (score_scale * LOG2E)
        o = qd_ref[:, (group + h) * HD:(group + h + 1) * HD]
        qh, ql = split(q)
        oh, ol = split(o)
        rhs_q.append(jnp.concatenate([qh, ql], axis=1))
        rhs_o.append(jnp.concatenate([oh, ol], axis=1))
        qth, qtl = split(q.T)
        oth, otl = split(o.T)
        qth2 = jnp.concatenate([qth, qth], axis=0)
        qtl2 = jnp.concatenate([qtl, qtl], axis=0)
        oth2 = jnp.concatenate([oth, oth], axis=0)
        otl2 = jnp.concatenate([otl, otl], axis=0)
        top = jnp.full((8, QT), -jnp.inf, f32)
        top_far = jnp.full((8, QT), -jnp.inf, f32)
        for c in range(0, span, KC):
            ka = kaug[pl.ds(a + c, KC), :]
            s = dot(ka, qth2) + dot(ka, qtl2)
            if c < QT:
                s = jnp.where(rows + c > cols, s, -jnp.inf)
            elif c >= tokens:
                s = jnp.where(rows + (c - tokens) <= cols, s, -jnp.inf)
            sref[pl.ds(c, KC), :] = s
            part = fold8(s, jnp.max)
            is_far = t + c // QT < far_tiles
            top = jnp.maximum(top, jnp.where(jnp.logical_and(first, is_far), -jnp.inf, part))
        m = jnp.max(top, axis=0, keepdims=True)
        total = jnp.zeros((8, QT), f32)
        dots = jnp.zeros((8, QT), f32)
        for c in range(0, span, KC):
            va = vaug[pl.ds(a + c, KC), :]
            dp = dot(va, oth2) + dot(va, otl2)
            is_far = t + c // QT < far_tiles
            shift = jnp.where(jnp.logical_and(first, is_far), BIG, m)
            p = jnp.exp2(sref[pl.ds(c, KC), :] - shift)
            total = total + fold8(p, jnp.sum)
            dots = dots + fold8(p * dp, jnp.sum)
            pref[pl.ds(c, KC), :] = p
            dpref[pl.ds(c, KC), :] = dp
        inv = 1.0 / jnp.sum(total, axis=0, keepdims=True)
        rd = jnp.sum(dots, axis=0, keepdims=True) * inv
        lanes = slice(h * QT, (h + 1) * QT)
        for c in range(0, span, KC):
            p = pref[pl.ds(c, KC), :] * inv
            ds = p * (dpref[pl.ds(c, KC), :] - rd)
            hi, lo = split(p)
            phi[pl.ds(c, KC), lanes] = hi
            plo[pl.ds(c, KC), lanes] = lo
            hi, lo = split(ds)
            dshi[pl.ds(c, KC), lanes] = hi
            dslo[pl.ds(c, KC), lanes] = lo
    oo = jnp.concatenate(rhs_o, axis=0)
    qq = jnp.concatenate(rhs_q, axis=0)
    for c in range(0, span, QT):
        dvacc[pl.ds(a + c, QT), :] += dot(phi[pl.ds(c, QT), :], oo) + dot(plo[pl.ds(c, QT), :], oo)
        dkacc[pl.ds(a + c, QT), :] += dot(dshi[pl.ds(c, QT), :], qq) + dot(dslo[pl.ds(c, QT), :], qq)
    kts = kt[:, pl.ds(a, span)]
    for h in range(group):
        lanes = slice(h * QT, (h + 1) * QT)
        full = dot(kts, dshi[:, lanes]) + dot(kts, dslo[:, lanes])
        dqt = (full[:HD] + full[HD:]) * score_scale
        dq_ref[:, h * HD:(h + 1) * HD] = dqt.T

    @pl.when(t == pl.num_programs(0) - 1)
    def _():
        for base, ref in ((0, dfar_ref), (tokens, down_ref)):
            for r in range(0, tokens, KC):
                dk = dkacc[pl.ds(base + r, KC), :]
                dv = dvacc[pl.ds(base + r, KC), :]
                ref[pl.ds(r, KC), :HD] = (dk[:, :HD] + dk[:, HD:]) * (1.0 / LOG2E)
                ref[pl.ds(r, KC), HD:] = dv[:, :HD] + dv[:, HD:]


def attn(first, qd, own, far, group):
    tokens = own.shape[0]
    span = tokens + QT
    whole = pl.BlockSpec((tokens, 2 * HD), lambda t: (0, 0))
    return pl.pallas_call(
        functools.partial(attn_kernel, group),
        grid=(tokens // QT,),
        in_specs=[
            pl.BlockSpec(memory_space=pltpu.SMEM),
            pl.BlockSpec((QT, 2 * group * HD), lambda t: (t, 0)),
            whole,
            whole,
        ],
        out_specs=[pl.BlockSpec((QT, group * HD), lambda t: (t, 0)), whole, whole],
        out_shape=[
            jax.ShapeDtypeStruct((tokens, group * HD), f32),
            jax.ShapeDtypeStruct((tokens, 2 * HD), f32),
            jax.ShapeDtypeStruct((tokens, 2 * HD), f32),
        ],
        scratch_shapes=[
            pltpu.VMEM((2 * tokens, 2 * HD), bf16),
            pltpu.VMEM((2 * tokens, 2 * HD), bf16),
            pltpu.VMEM((2 * HD, 2 * tokens), bf16),
            pltpu.VMEM((2 * tokens, 2 * HD), f32),
            pltpu.VMEM((2 * tokens, 2 * HD), f32),
            pltpu.VMEM((span, QT), f32),
            pltpu.VMEM((span, QT), f32),
            pltpu.VMEM((span, QT), f32),
            pltpu.VMEM((span, group * QT), bf16),
            pltpu.VMEM((span, group * QT), bf16),
            pltpu.VMEM((span, group * QT), bf16),
            pltpu.VMEM((span, group * QT), bf16),
        ],
        compiler_params=pltpu.CompilerParams(dimension_semantics=("arbitrary",)),
        name="attn",
    )(first, qd, own, far)


def pack_kernel(a_ref, b_ref, out_ref):
    width = a_ref.shape[1]
    out_ref[0, :, :width] = a_ref[...]
    out_ref[0, :, width:] = b_ref[...]


def pack(a, b, parts):
    rows, cols = a.shape
    width = cols // parts
    spec = pl.BlockSpec((rows, width), lambda j: (0, j))
    return pl.pallas_call(
        pack_kernel,
        grid=(parts,),
        in_specs=[spec, spec],
        out_specs=pl.BlockSpec((1, rows, 2 * width), lambda j: (j, 0, 0)),
        out_shape=jax.ShapeDtypeStruct((parts, rows, 2 * width), a.dtype),
        name="pack",
    )(a, b)


def unpack_kernel(x_ref, *outs):
    width = x_ref.shape[2] // len(outs)
    for n, out_ref in enumerate(outs):
        out_ref[...] = x_ref[0, :, n * width:(n + 1) * width]


def unpack(x, count):
    parts, rows, cols = x.shape
    width = cols // count
    spec = pl.BlockSpec((rows, width), lambda j: (0, j))
    return pl.pallas_call(
        unpack_kernel,
        grid=(parts,),
        in_specs=[pl.BlockSpec((1, rows, cols), lambda j: (j, 0, 0))],
        out_specs=[spec] * count,
        out_shape=[jax.ShapeDtypeStruct((rows, parts * width), x.dtype)] * count,
        name="unpack",
    )(x)


PLANE = ("inner", "head")


def swap(x):
    return lax.all_to_all(x, PLANE, split_axis=0, concat_axis=0, tiled=True)


def shifted(x, by):
    devices = lax.axis_size("outer")
    return lax.ppermute(x, "outer", [(i, i + by) for i in range(devices) if 0 <= i + by < devices])


def per_device(query, key_in, value_in, d_out):
    parts = lax.axis_size("inner") * lax.axis_size("head")
    rows = query.shape[0]
    group = query.shape[1] // key_in.shape[1]
    assert key_in.shape[1] == parts * HD
    tokens = rows * parts
    first = (lax.axis_index("outer") == 0).astype(jnp.int32).reshape(1)
    own = swap(pack(key_in, value_in, parts)).reshape(tokens, 2 * HD)
    qd = swap(pack(query, d_out, parts)).reshape(tokens, 2 * group * HD)
    far = shifted(own, 1)
    dq, down, dfar = attn(first, qd, own, far, group)
    back_q = swap(dq.reshape(parts, rows, group * HD))
    total = down + shifted(dfar, -1)
    back_kv = swap(total.reshape(parts, rows, 2 * HD))
    (grad_query,) = unpack(back_q, 1)
    grad_key, grad_value = unpack(back_kv, 2)
    return grad_query, grad_key, grad_value


def solution(mesh):
    assert mesh.axis_names == ("head", "seq")
    heads, seqs = mesh.devices.shape

    def run(query, key_in, value_in, d_out):
        shard = query.shape[0] // seqs
        inner = WINDOW // shard
        fine = jax.sharding.Mesh(
            mesh.devices.reshape(heads, seqs // inner, inner), ("head", "outer", "inner")
        )
        spec = P(("outer", "inner", "head"), None)
        return jax.shard_map(
            per_device, mesh=fine, in_specs=(spec,) * 4, out_specs=(spec,) * 3, check_vma=False
        )(query, key_in, value_in, d_out)

    return run
```

```python
import functools
import math

import jax
import jax.numpy as jnp
from jax import lax
from jax.experimental import pallas as pl
from jax.experimental.pallas import tpu as pltpu
from jax.sharding import PartitionSpec as P


HD = 128
WINDOW = 1024
KC = 128

score_scale = 168.0 ** (-0.5)
LOG2E = 1.0 / math.log(2.0)
f32 = jnp.float32
bf16 = jnp.bfloat16
BIG = 3.0e38
ATTN_VMEM = 36 << 20
MOVE_VMEM = 10 << 20


def split(x):
    hi = x.astype(bf16)
    lo = (x - hi.astype(f32)).astype(bf16)
    return hi, lo


def dot(a, b):
    return jnp.dot(a, b, preferred_element_type=f32)


def fold8(x, op):
    rows, cols = x.shape
    return op(x.reshape(rows // 8, 8, cols), axis=0)


QB = 128
KC = 64


def attn_kernel(
    group, stage, parts, carried, place_ref, *refs,
):
    blocks, refs = refs[:parts], refs[parts:]
    own, refs = refs[:parts], refs[parts:]
    near, rest, refs = refs[0], refs[1], refs[2:]
    given, refs = refs[:carried], refs[carried:]
    dq_ref, refs = refs[0], refs[1:]
    grads, refs = refs[:3], refs[3:]
    kaug, vaug, kt, dkacc, dvacc, sref, dpref = refs[:7]
    bufs, qbuf = refs[7:-1], refs[-1]
    me = place_ref[1]
    u = pl.program_id(0)
    steps = pl.num_programs(0)
    tokens = parts * QB
    half = tokens // 2
    done_rows = stage * half
    span = tokens + QB
    far_tiles = parts - stage * (parts // 2)
    lanes = group * QB
    sets = (bufs[:6], bufs[6:])
    first = place_ref[0] == 0

    @pl.when(u == 0)
    def _():
        count = parts // 2
        same = (me < count) == (stage == 0)

        def far_block(k):
            return near[k] if k < near.shape[0] else rest[k - near.shape[0]]

        def own_block(k):
            return own[k][...]

        def place_keys(kv, r):
            r = pl.multiple_of(r, QB)
            k = kv[:, :HD]
            hi, lo = split(k)
            kaug[pl.ds(r, QB), :HD] = hi
            kaug[pl.ds(r, QB), HD:] = lo
            vh, vl = split(kv[:, HD:])
            vaug[pl.ds(r, QB), :HD] = vh
            vaug[pl.ds(r, QB), HD:] = vl
            th, tl = split(k.T)
            kt[:HD, pl.ds(r, QB)] = th
            kt[HD:, pl.ds(r, QB)] = tl

        full, part = (far_block, own_block) if stage == 0 else (own_block, far_block)
        full_base, part_base = (0, tokens) if stage == 0 else (half, 0)
        for k in range(parts):
            place_keys(full(k), full_base + (me ^ k) * QB)
        for j in range(count):
            slot = (me ^ j) & (count - 1)
            place_keys(jnp.where(same, part(j), part(count + j)), part_base + slot * QB)
            qbuf[slot] = jnp.where(same, blocks[j][...], blocks[count + j][...])
        dkacc[...] = jnp.zeros_like(dkacc)
        dvacc[...] = jnp.zeros_like(dvacc)
        for buf in sets[1]:
            buf[...] = jnp.zeros_like(buf)
        if done_rows:
            dq_ref[:done_rows, :] = given[-1][...]

    rows = lax.broadcasted_iota(jnp.int32, (KC, lanes), 0)
    cols = lax.rem(lax.broadcasted_iota(jnp.int32, (KC, lanes), 1), QB)

    def products(tile, buf):
        phi, plo, dshi, dslo, qq, oo = buf
        a = pl.multiple_of(jnp.maximum(tile, 0) * QB, QB)
        q2 = qq[...]
        o2 = oo[...]
        for c in range(0, span, 192):
            dvacc[pl.ds(a + c, 192), :] += dot(phi[c:c + 192, :], o2) + dot(plo[c:c + 192, :], o2)
        for c in range(0, span, 192):
            dkacc[pl.ds(a + c, 192), :] += dot(dshi[c:c + 192, :], q2) + dot(dslo[c:c + 192, :], q2)
        kts = kt[:, pl.ds(a, span)]
        full = dot(kts, dshi[...]) + dot(kts, dslo[...])
        dqt = (full[:HD] + full[HD:]) * score_scale
        for h in range(group):
            dq_ref[pl.ds(done_rows + a, QB), h * HD:(h + 1) * HD] = dqt[:, h * QB:(h + 1) * QB].T

    def weights(tile, buf):
        slot = tile
        phi, plo, dshi, dslo, qq, oo = buf
        a = pl.multiple_of(tile * QB, QB)
        qts = []
        ots = []
        for h in range(group):
            q = qbuf[slot, :, h * HD:(h + 1) * HD] * (score_scale * LOG2E)
            o = qbuf[slot, :, (group + h) * HD:(group + h + 1) * HD]
            qh, ql = split(q)
            oh, ol = split(o)
            qq[h * QB:(h + 1) * QB, :HD] = qh
            qq[h * QB:(h + 1) * QB, HD:] = ql
            oo[h * QB:(h + 1) * QB, :HD] = oh
            oo[h * QB:(h + 1) * QB, HD:] = ol
            qts.append(q.T)
            ots.append(o.T)
        qth, qtl = split(jnp.concatenate(qts, axis=1))
        oth, otl = split(jnp.concatenate(ots, axis=1))
        qhh = jnp.concatenate([qth, qth], axis=0)
        qll = jnp.concatenate([qtl, qtl], axis=0)
        ohh = jnp.concatenate([oth, oth], axis=0)
        oll = jnp.concatenate([otl, otl], axis=0)
        for c in range(0, span, 192):
            ka = kaug[pl.ds(a + c, 192), :]
            sref[c:c + 192, :] = dot(ka, qhh) + dot(ka, qll)
        for c in range(0, span, 192):
            va = vaug[pl.ds(a + c, 192), :]
            dpref[c:c + 192, :] = dot(va, ohh) + dot(va, oll)

        def masked(c):
            s = sref[c:c + KC, :]
            if c < QB:
                s = jnp.where(rows + c > cols, s, -jnp.inf)
            elif c >= tokens:
                s = jnp.where(rows + (c - tokens) <= cols, s, -jnp.inf)
            return s

        def is_far(c):
            return jnp.logical_and(first, tile + c // QB < far_tiles)

        top = jnp.full((8, lanes), -jnp.inf, f32)
        for b in range(0, span, QB):
            part = jnp.full((8, lanes), -jnp.inf, f32)
            for c in range(b, b + QB, KC):
                part = jnp.maximum(part, fold8(masked(c), jnp.max))
            top = jnp.maximum(top, jnp.where(is_far(b), -jnp.inf, part))
        m = jnp.max(top, axis=0, keepdims=True)
        total = jnp.zeros((8, lanes), f32)
        dots = jnp.zeros((8, lanes), f32)
        for c in range(0, span, KC):
            shift = jnp.where(is_far(c), BIG, m)
            p = jnp.exp2(masked(c) - shift)
            total = total + fold8(p, jnp.sum)
            dots = dots + fold8(p * dpref[c:c + KC, :], jnp.sum)
            sref[c:c + KC, :] = p
        inv = 1.0 / jnp.sum(total, axis=0, keepdims=True)
        rd = jnp.sum(dots, axis=0, keepdims=True) * inv
        for c in range(0, span, KC):
            p = sref[c:c + KC, :] * inv
            ds = p * (dpref[c:c + KC, :] - rd)
            hi, lo = split(p)
            phi[c:c + KC, :] = hi
            plo[c:c + KC, :] = lo
            hi, lo = split(ds)
            dshi[c:c + KC, :] = hi
            dslo[c:c + KC, :] = lo

    for n in range(2):
        tile = 2 * u + n
        products(tile - 1, sets[1 - n])
        weights(tile, sets[n])

    @pl.when(u == steps - 1)
    def _():
        products(2 * u + 1, sets[1])
        for n, ref in enumerate(grads):
            base = n * half
            for r in range(0, half, QB):
                dk = dkacc[pl.ds(base + r, QB), :]
                dv = dvacc[pl.ds(base + r, QB), :]
                dk = (dk[:, :HD] + dk[:, HD:]) * (1.0 / LOG2E)
                dv = dv[:, :HD] + dv[:, HD:]
                if n < carried - 1:
                    dk = dk + given[n][pl.ds(r, QB), :HD]
                    dv = dv + given[n][pl.ds(r, QB), HD:]
                ref[pl.ds(r, QB), :HD] = dk
                ref[pl.ds(r, QB), HD:] = dv


def attn(place, blocks, part, far, own, given, group):
    half = len(own) * QB // 2
    span = 2 * half + QB
    lanes = group * QB
    tiles = half // QB
    assert blocks[0].shape[0] == QB
    whole = pl.BlockSpec((half, 2 * HD), lambda t, s: (0, 0))
    pick = [pl.BlockSpec(x.shape, lambda t, s, n=x.ndim: (0,) * n) for x in (*own, *far)]
    buf = [pltpu.VMEM((span, lanes), bf16)] * 4 + [pltpu.VMEM((lanes, 2 * HD), bf16)] * 2
    dq_shape = ((1 + part) * half, group * HD)
    return pl.pallas_call(
        functools.partial(attn_kernel, group, part, len(blocks), len(given)),
        grid_spec=pltpu.PrefetchScalarGridSpec(
            num_scalar_prefetch=1,
            grid=(tiles // 2,),
            in_specs=[
                *[pl.BlockSpec(x.shape, lambda t, s: (0, 0)) for x in blocks],
                *pick, *[pl.BlockSpec(x.shape, lambda t, s: (0, 0)) for x in given],
            ],
            out_specs=[pl.BlockSpec(dq_shape, lambda t, s: (0, 0)), whole, whole, whole],
            scratch_shapes=[
                pltpu.VMEM((3 * half, 2 * HD), bf16),
                pltpu.VMEM((3 * half, 2 * HD), bf16),
                pltpu.VMEM((2 * HD, 3 * half), bf16),
                pltpu.VMEM((3 * half, 2 * HD), f32),
                pltpu.VMEM((3 * half, 2 * HD), f32),
                pltpu.VMEM((span, lanes), f32),
                pltpu.VMEM((span, lanes), f32),
                *buf,
                *buf,
                pltpu.VMEM((tiles, *blocks[0].shape), f32),
            ],
        ),
        out_shape=[
            jax.ShapeDtypeStruct(dq_shape, f32),
            *[jax.ShapeDtypeStruct((half, 2 * HD), f32)] * 3,
        ],
        compiler_params=pltpu.CompilerParams(
            dimension_semantics=("arbitrary",), vmem_limit_bytes=ATTN_VMEM),
    )(place, *blocks, *own, *far, *given)


def spread_kernel(parts, place_ref, *refs):
    ins, outs, sems = refs[:2], refs[2:-1], refs[-1]
    me = place_ref[1]
    copies = []
    for k in range(parts):
        for n, ref in enumerate(ins):
            width = ref.shape[1] // parts
            start = pl.multiple_of((me ^ k) * width, width)
            copies.append(pltpu.make_async_copy(
                ref.at[:, pl.ds(start, width)],
                outs[k].at[:, pl.ds(n * width, width)],
                sems.at[2 * k + n],
            ))
    for copy in copies:
        copy.start()
    for copy in copies:
        copy.wait()


def spread(place, first, second, parts):
    rows, cols = first.shape
    return pl.pallas_call(
        functools.partial(spread_kernel, parts),
        in_specs=[
            pl.BlockSpec(memory_space=pltpu.SMEM),
            pl.BlockSpec(memory_space=pltpu.MemorySpace.HBM),
            pl.BlockSpec(memory_space=pltpu.MemorySpace.HBM),
        ],
        out_specs=[pl.BlockSpec(memory_space=pltpu.VMEM)] * parts,
        out_shape=[jax.ShapeDtypeStruct((rows, 2 * cols // parts), f32)] * parts,
        scratch_shapes=[pltpu.SemaphoreType.DMA((2 * parts,))],
        compiler_params=pltpu.CompilerParams(vmem_limit_bytes=MOVE_VMEM),
    )(place, first, second)


def combine_kernel(place_ref, own_ref, back_ref, *outs):
    me = place_ref[1]
    count = len(outs)
    for j, out in enumerate(outs):
        rows = out.shape[0]
        r = pl.ds(pl.multiple_of(((me ^ j) & (count - 1)) * rows, rows), rows)
        out[...] = own_ref[r, :] + back_ref[r, :]


def combine(place, own, back, count):
    rows, cols = own.shape
    vmem = pl.BlockSpec(memory_space=pltpu.VMEM)
    return pl.pallas_call(
        combine_kernel,
        in_specs=[pl.BlockSpec(memory_space=pltpu.SMEM), vmem, vmem],
        out_specs=[vmem] * count,
        out_shape=[jax.ShapeDtypeStruct((rows // count, cols), f32)] * count,
        compiler_params=pltpu.CompilerParams(vmem_limit_bytes=MOVE_VMEM),
    )(place, own, back)


def unpack_q_kernel(x_ref, out_ref):
    width = x_ref.shape[2]
    for j in range(x_ref.shape[0]):
        out_ref[:, j * width:(j + 1) * width] = x_ref[j]


def unpack_q(x):
    parts, rows, cols = x.shape
    return pl.pallas_call(
        unpack_q_kernel,
        out_shape=jax.ShapeDtypeStruct((rows, parts * cols), f32),
        compiler_params=pltpu.CompilerParams(vmem_limit_bytes=MOVE_VMEM),
        name="unpack_q",
    )(x)


def gather_kernel(parts, place_ref, *refs):
    sets, outs = (refs[:parts], refs[parts:2 * parts]), refs[2 * parts:]
    me = place_ref[1]
    upper = me >= parts // 2
    for n, blocks in enumerate(sets):
        @pl.when(upper if n else jnp.logical_not(upper))
        def _():
            for k, block in enumerate(blocks):
                start = pl.multiple_of((me ^ k) * HD, HD)
                for m, out in enumerate(outs):
                    out[:, pl.ds(start, HD)] = block[:, m * HD:(m + 1) * HD]


def gather(place, lower, upper):
    parts = len(lower)
    rows, _ = lower[0].shape
    vmem = pl.BlockSpec(memory_space=pltpu.VMEM)
    return pl.pallas_call(
        functools.partial(gather_kernel, parts),
        in_specs=[pl.BlockSpec(memory_space=pltpu.SMEM)] + [vmem] * (2 * parts),
        out_specs=[vmem] * 2,
        out_shape=[jax.ShapeDtypeStruct((rows, parts * HD), f32)] * 2,
        compiler_params=pltpu.CompilerParams(vmem_limit_bytes=MOVE_VMEM),
        name="unpack_kv",
    )(place, *lower, *upper)


PLANE = ("inner", "head")


def swap(x):
    return lax.all_to_all(x, PLANE, split_axis=0, concat_axis=0, tiled=True)


def shifted(x, by):
    devices = lax.axis_size("outer")
    return lax.ppermute(x, "outer", [(i, i + by) for i in range(devices) if 0 <= i + by < devices])


def exchanged(x, k, side=None):
    heads, inner = lax.axis_size("head"), lax.axis_size("inner")
    pairs = []
    for h in range(heads):
        for i in range(inner):
            to = (i * heads + h) ^ k
            if side is None or to // heads == side:
                pairs.append((h * inner + i, (to % heads) * inner + to // heads))
    return lax.ppermute(x, ("head", "inner"), pairs)


def staged(query, key_in, value_in, d_out):
    heads = lax.axis_size("head")
    parts = lax.axis_size("inner") * heads
    rows = query.shape[0]
    group = query.shape[1] // key_in.shape[1]
    assert lax.axis_size("inner") == 2 and heads & (heads - 1) == 0
    assert key_in.shape[1] == parts * HD and rows == QB
    me = lax.axis_index("inner") * heads + lax.axis_index("head")
    place = jnp.stack([lax.axis_index("outer"), me]).astype(jnp.int32)
    order = range(parts - 1, 0, -1)
    kv = list(spread(place, key_in, value_in, parts))
    for k in order:
        kv[k] = exchanged(kv[k], k)
    blocks = list(spread(place, query, d_out, parts))
    for k in order:
        blocks[k] = exchanged(blocks[k], k)
    near = shifted(jnp.stack(kv[:2]), 1)
    rest = shifted(jnp.stack(kv[2:]), 1)
    far, own = (near, rest), kv
    dq0, f0, f1, o0 = attn(place, blocks, 0, far, own, (), group)
    back0 = shifted(f0, -1)
    dq, f1, o0, o1 = attn(place, blocks, 1, far, own, (f1, o0, dq0), group)
    back1 = shifted(f1, -1)
    back_q = swap(dq.reshape(parts, rows, group * HD))
    sides = []
    for side, (mine, back) in enumerate(((o0, back0), (o1, back1))):
        sums = combine(place, mine, back, heads)
        got = [sums[0]]
        for k in range(1, parts):
            got.append(exchanged(sums[k % heads], k, side))
        sides.append(got)
    grad_query = unpack_q(back_q)
    grad_key, grad_value = gather(place, *sides)
    return grad_query, grad_key, grad_value


def solution(mesh):
    assert mesh.axis_names == ("head", "seq")
    heads, seqs = mesh.devices.shape

    def run(query, key_in, value_in, d_out):
        shard = query.shape[0] // seqs
        inner = WINDOW // shard
        fine = jax.sharding.Mesh(
            mesh.devices.reshape(heads, seqs // inner, inner), ("head", "outer", "inner")
        )
        spec = P(("outer", "inner", "head"), None)
        step = jax.shard_map(
            staged, mesh=fine, in_specs=(spec,) * 4, out_specs=(spec,) * 3, check_vma=False
        )
        return step(query, key_in, value_in, d_out)

    return run
```

```python
import functools
import math

import jax
import jax.numpy as jnp
from jax import lax
from jax.experimental import pallas as pl
from jax.experimental.pallas import tpu as pltpu
from jax.sharding import PartitionSpec as P


HD = 128
WINDOW = 1024
KC = 128

score_scale = 168.0 ** (-0.5)
LOG2E = 1.0 / math.log(2.0)
f32 = jnp.float32
bf16 = jnp.bfloat16
BIG = 3.0e38
ATTN_VMEM = 36 << 20
MOVE_VMEM = 10 << 20


def split(x):
    hi = x.astype(bf16)
    lo = (x - hi.astype(f32)).astype(bf16)
    return hi, lo


def dot(a, b):
    return jnp.dot(a, b, preferred_element_type=f32)


def fold8(x, op):
    rows, cols = x.shape
    return op(x.reshape(rows // 8, 8, cols), axis=0)


QB = 128
KC = 64
MC = 192
PC = 256


def attn_kernel(group, stage, parts, carried, place_ref, *refs):
    blocks, refs = refs[:parts], refs[parts:]
    own, refs = refs[:parts], refs[parts:]
    near, rest, refs = refs[0], refs[1], refs[2:]
    given, refs = refs[:carried], refs[carried:]
    dq_ref, refs = refs[0], refs[1:]
    grads, refs = refs[:3], refs[3:]
    kaug, vaug, kt, dkacc, dvacc, qbuf, qall, oall = refs[:8]
    refs = refs[8:]
    size = len(refs) // 2
    sets = (refs[:size], refs[size:])
    me = place_ref[1]
    first = place_ref[0] == 0
    tokens = parts * QB
    half = tokens // 2
    count = parts // 2
    done_rows = stage * half
    span = tokens + QB
    far_tiles = parts - stage * count
    lanes = group * QB
    same = (me < count) == (stage == 0)

    def far_block(k):
        return near[k] if k < near.shape[0] else rest[k - near.shape[0]]

    def own_block(k):
        return own[k][...]

    def place_keys(kv, r):
        r = pl.multiple_of(r, QB)
        k = kv[:, :HD]
        hi, lo = split(k)
        kaug[pl.ds(r, QB), :HD] = hi
        kaug[pl.ds(r, QB), HD:] = lo
        vh, vl = split(kv[:, HD:])
        vaug[pl.ds(r, QB), :HD] = vh
        vaug[pl.ds(r, QB), HD:] = vl
        th, tl = split(k.T)
        kt[:HD, pl.ds(r, QB)] = th
        kt[HD:, pl.ds(r, QB)] = tl

    full, part = (far_block, own_block) if stage == 0 else (own_block, far_block)
    full_base, part_base = (0, tokens) if stage == 0 else (half, 0)
    for k in range(parts):
        place_keys(full(k), full_base + (me ^ k) * QB)
    for j in range(count):
        slot = (me ^ j) & (count - 1)
        place_keys(jnp.where(same, part(j), part(count + j)), part_base + slot * QB)
        qbuf[slot] = jnp.where(same, blocks[j][...], blocks[count + j][...])
    if done_rows:
        dq_ref[:done_rows, :] = given[-1][...]

    rows = lax.broadcasted_iota(jnp.int32, (KC, lanes), 0)
    cols = lax.rem(lax.broadcasted_iota(jnp.int32, (KC, lanes), 1), QB)

    def scores(tile):
        sref, dpref = sets[tile % 2][:2]
        qq, oo = qall.at[tile], oall.at[tile]
        a = tile * QB
        qts = []
        ots = []
        for h in range(group):
            q = qbuf[tile, :, h * HD:(h + 1) * HD] * (score_scale * LOG2E)
            o = qbuf[tile, :, (group + h) * HD:(group + h + 1) * HD]
            qh, ql = split(q)
            oh, ol = split(o)
            qq[h * QB:(h + 1) * QB, :HD] = qh
            qq[h * QB:(h + 1) * QB, HD:] = ql
            oo[h * QB:(h + 1) * QB, :HD] = oh
            oo[h * QB:(h + 1) * QB, HD:] = ol
            qts.append(q.T)
            ots.append(o.T)
        qth, qtl = split(jnp.concatenate(qts, axis=1))
        oth, otl = split(jnp.concatenate(ots, axis=1))
        qhh = jnp.concatenate([qth, qth], axis=0)
        qll = jnp.concatenate([qtl, qtl], axis=0)
        ohh = jnp.concatenate([oth, oth], axis=0)
        oll = jnp.concatenate([otl, otl], axis=0)
        for c in range(0, span, MC):
            ka = kaug[a + c:a + c + MC, :]
            sref[c:c + MC, :] = dot(ka, qhh) + dot(ka, qll)
        for c in range(0, span, MC):
            va = vaug[a + c:a + c + MC, :]
            dpref[c:c + MC, :] = dot(va, ohh) + dot(va, oll)

    def softmax(tile):
        sref, dpref, phi, plo, dshi, dslo = sets[tile % 2]

        def masked(c):
            s = sref[c:c + KC, :]
            if c < QB:
                s = jnp.where(rows + c > cols, s, -jnp.inf)
            elif c >= tokens:
                s = jnp.where(rows + (c - tokens) <= cols, s, -jnp.inf)
            return s

        border = (far_tiles - tile) * QB
        tops = []
        for lo, hi in ((0, border), (border, span)):
            top = jnp.full((8, lanes), -jnp.inf, f32)
            for c in range(lo, hi, KC):
                top = jnp.maximum(top, fold8(masked(c), jnp.max))
            tops.append(jnp.max(top, axis=0, keepdims=True))
        m = jnp.maximum(tops[1], jnp.where(first, -jnp.inf, tops[0]))
        far_m = jnp.where(first, BIG, m)
        total = jnp.zeros((8, lanes), f32)
        dots = jnp.zeros((8, lanes), f32)
        for c in range(0, span, KC):
            p = jnp.exp2(masked(c) - (far_m if c < border else m))
            total = total + fold8(p, jnp.sum)
            dots = dots + fold8(p * dpref[c:c + KC, :], jnp.sum)
            sref[c:c + KC, :] = p
        inv = 1.0 / jnp.sum(total, axis=0, keepdims=True)
        rd = jnp.sum(dots, axis=0, keepdims=True) * inv
        for c in range(0, span, KC):
            p = sref[c:c + KC, :] * inv
            ds = p * (dpref[c:c + KC, :] - rd)
            hi, lo = split(p)
            phi[c:c + KC, :] = hi
            plo[c:c + KC, :] = lo
            hi, lo = split(ds)
            dshi[c:c + KC, :] = hi
            dslo[c:c + KC, :] = lo

    def products(tile):
        phi, plo, dshi, dslo = sets[tile % 2][2:]
        a = tile * QB
        q2 = qall[tile]
        o2 = oall[tile]
        pieces = [(c, PC) for c in range(0, tokens, PC)] + [(tokens, QB)]
        for acc, high, low, rhs in ((dvacc, phi, plo, o2), (dkacc, dshi, dslo, q2)):
            for c, n in pieces:
                value = dot(high[c:c + n, :], rhs) + dot(low[c:c + n, :], rhs)
                if tile and c < tokens:
                    acc[a + c:a + c + n, :] += value
                else:
                    acc[a + c:a + c + n, :] = value
        kts = kt[:, a:a + span]
        both = dot(kts, dshi[...]) + dot(kts, dslo[...])
        dqt = (both[:HD] + both[HD:]) * score_scale
        for h in range(group):
            dq_ref[done_rows + a:done_rows + a + QB, h * HD:(h + 1) * HD] = (
                dqt[:, h * QB:(h + 1) * QB].T)

    def finish(r):
        n, row = r // half, r % half
        dk = dkacc[r:r + QB, :]
        dv = dvacc[r:r + QB, :]
        dk = (dk[:, :HD] + dk[:, HD:]) * (1.0 / LOG2E)
        dv = dv[:, :HD] + dv[:, HD:]
        if n < carried - 1:
            dk = dk + given[n][row:row + QB, :HD]
            dv = dv + given[n][row:row + QB, HD:]
        grads[n][row:row + QB, :HD] = dk
        grads[n][row:row + QB, HD:] = dv

    scores(0)
    for tile in range(count):
        if tile + 1 < count:
            scores(tile + 1)
        if tile:
            products(tile - 1)
        softmax(tile)
    products(count - 1)
    for r in range(0, tokens + half, QB):
        finish(r)


def attn(place, blocks, part, far, own, given, group):
    half = len(own) * QB // 2
    span = 2 * half + QB
    lanes = group * QB
    tiles = half // QB
    assert blocks[0].shape[0] == QB
    vmem = pl.BlockSpec(memory_space=pltpu.VMEM)
    dq_shape = ((1 + part) * half, group * HD)
    buf = (
        [pltpu.VMEM((span, lanes), f32)] * 2
        + [pltpu.VMEM((span, lanes), bf16)] * 4
    )
    operands = (*blocks, *own, *far, *given)
    return pl.pallas_call(
        functools.partial(attn_kernel, group, part, len(blocks), len(given)),
        in_specs=[pl.BlockSpec(memory_space=pltpu.SMEM)] + [vmem] * len(operands),
        out_specs=[vmem] * 4,
        scratch_shapes=[
            pltpu.VMEM((3 * half, 2 * HD), bf16),
            pltpu.VMEM((3 * half, 2 * HD), bf16),
            pltpu.VMEM((2 * HD, 3 * half), bf16),
            pltpu.VMEM((3 * half, 2 * HD), f32),
            pltpu.VMEM((3 * half, 2 * HD), f32),
            pltpu.VMEM((tiles, *blocks[0].shape), f32),
            pltpu.VMEM((tiles, lanes, 2 * HD), bf16),
            pltpu.VMEM((tiles, lanes, 2 * HD), bf16),
            *buf,
            *buf,
        ],
        out_shape=[
            jax.ShapeDtypeStruct(dq_shape, f32),
            *[jax.ShapeDtypeStruct((half, 2 * HD), f32)] * 3,
        ],
        compiler_params=pltpu.CompilerParams(vmem_limit_bytes=ATTN_VMEM),
    )(place, *operands)


def spread_kernel(parts, place_ref, *refs):
    ins, outs, sems = refs[:2], refs[2:-1], refs[-1]
    me = place_ref[1]
    copies = []
    for k in range(parts):
        for n, ref in enumerate(ins):
            width = ref.shape[1] // parts
            start = pl.multiple_of((me ^ k) * width, width)
            copies.append(pltpu.make_async_copy(
                ref.at[:, pl.ds(start, width)],
                outs[k].at[:, pl.ds(n * width, width)],
                sems.at[2 * k + n],
            ))
    for copy in copies:
        copy.start()
    for copy in copies:
        copy.wait()


def spread(place, first, second, parts):
    rows, cols = first.shape
    return pl.pallas_call(
        functools.partial(spread_kernel, parts),
        in_specs=[
            pl.BlockSpec(memory_space=pltpu.SMEM),
            pl.BlockSpec(memory_space=pltpu.MemorySpace.HBM),
            pl.BlockSpec(memory_space=pltpu.MemorySpace.HBM),
        ],
        out_specs=[pl.BlockSpec(memory_space=pltpu.VMEM)] * parts,
        out_shape=[jax.ShapeDtypeStruct((rows, 2 * cols // parts), f32)] * parts,
        scratch_shapes=[pltpu.SemaphoreType.DMA((2 * parts,))],
        compiler_params=pltpu.CompilerParams(vmem_limit_bytes=MOVE_VMEM),
    )(place, first, second)


def combine_kernel(place_ref, own_ref, back_ref, *outs):
    me = place_ref[1]
    count = len(outs)
    for j, out in enumerate(outs):
        rows = out.shape[0]
        r = pl.ds(pl.multiple_of(((me ^ j) & (count - 1)) * rows, rows), rows)
        out[...] = own_ref[r, :] + back_ref[r, :]


def combine(place, own, back, count):
    rows, cols = own.shape
    vmem = pl.BlockSpec(memory_space=pltpu.VMEM)
    return pl.pallas_call(
        combine_kernel,
        in_specs=[pl.BlockSpec(memory_space=pltpu.SMEM), vmem, vmem],
        out_specs=[vmem] * count,
        out_shape=[jax.ShapeDtypeStruct((rows // count, cols), f32)] * count,
        compiler_params=pltpu.CompilerParams(vmem_limit_bytes=MOVE_VMEM),
    )(place, own, back)


def unpack_q_kernel(x_ref, out_ref):
    width = x_ref.shape[2]
    for j in range(x_ref.shape[0]):
        out_ref[:, j * width:(j + 1) * width] = x_ref[j]


def unpack_q(x):
    parts, rows, cols = x.shape
    return pl.pallas_call(
        unpack_q_kernel,
        out_shape=jax.ShapeDtypeStruct((rows, parts * cols), f32),
        compiler_params=pltpu.CompilerParams(vmem_limit_bytes=MOVE_VMEM),
        name="unpack_q",
    )(x)


def gather_kernel(parts, place_ref, *refs):
    sets, outs = (refs[:parts], refs[parts:2 * parts]), refs[2 * parts:]
    me = place_ref[1]
    upper = me >= parts // 2
    for n, blocks in enumerate(sets):
        @pl.when(upper if n else jnp.logical_not(upper))
        def _():
            for k, block in enumerate(blocks):
                start = pl.multiple_of((me ^ k) * HD, HD)
                for m, out in enumerate(outs):
                    out[:, pl.ds(start, HD)] = block[:, m * HD:(m + 1) * HD]


def gather(place, lower, upper):
    parts = len(lower)
    rows, _ = lower[0].shape
    vmem = pl.BlockSpec(memory_space=pltpu.VMEM)
    return pl.pallas_call(
        functools.partial(gather_kernel, parts),
        in_specs=[pl.BlockSpec(memory_space=pltpu.SMEM)] + [vmem] * (2 * parts),
        out_specs=[vmem] * 2,
        out_shape=[jax.ShapeDtypeStruct((rows, parts * HD), f32)] * 2,
        compiler_params=pltpu.CompilerParams(vmem_limit_bytes=MOVE_VMEM),
        name="unpack_kv",
    )(place, *lower, *upper)


PLANE = ("inner", "head")


def swap(x):
    return lax.all_to_all(x, PLANE, split_axis=0, concat_axis=0, tiled=True)


def shifted(x, by):
    devices = lax.axis_size("outer")
    return lax.ppermute(x, "outer", [(i, i + by) for i in range(devices) if 0 <= i + by < devices])


def exchanged(x, k, side=None):
    heads, inner = lax.axis_size("head"), lax.axis_size("inner")
    pairs = []
    for h in range(heads):
        for i in range(inner):
            to = (i * heads + h) ^ k
            if side is None or to // heads == side:
                pairs.append((h * inner + i, (to % heads) * inner + to // heads))
    return lax.ppermute(x, ("head", "inner"), pairs)


def staged(query, key_in, value_in, d_out):
    heads = lax.axis_size("head")
    parts = lax.axis_size("inner") * heads
    rows = query.shape[0]
    group = query.shape[1] // key_in.shape[1]
    assert lax.axis_size("inner") == 2 and heads & (heads - 1) == 0
    assert key_in.shape[1] == parts * HD and rows == QB
    me = lax.axis_index("inner") * heads + lax.axis_index("head")
    place = jnp.stack([lax.axis_index("outer"), me]).astype(jnp.int32)
    order = range(parts - 1, 0, -1)
    kv = list(spread(place, key_in, value_in, parts))
    for k in order:
        kv[k] = exchanged(kv[k], k)
    blocks = list(spread(place, query, d_out, parts))
    for k in order:
        blocks[k] = exchanged(blocks[k], k)
    near = shifted(jnp.stack(kv[:2]), 1)
    rest = shifted(jnp.stack(kv[2:]), 1)
    far, own = (near, rest), kv
    dq0, f0, f1, o0 = attn(place, blocks, 0, far, own, (), group)
    back0 = shifted(f0, -1)
    dq, f1, o0, o1 = attn(place, blocks, 1, far, own, (f1, o0, dq0), group)
    back1 = shifted(f1, -1)
    back_q = swap(dq.reshape(parts, rows, group * HD))
    sides = []
    for side, (mine, back) in enumerate(((o0, back0), (o1, back1))):
        sums = combine(place, mine, back, heads)
        got = [sums[0]]
        for k in range(1, parts):
            got.append(exchanged(sums[k % heads], k, side))
        sides.append(got)
    grad_query = unpack_q(back_q)
    grad_key, grad_value = gather(place, *sides)
    return grad_query, grad_key, grad_value


def solution(mesh):
    assert mesh.axis_names == ("head", "seq")
    heads, seqs = mesh.devices.shape

    def run(query, key_in, value_in, d_out):
        shard = query.shape[0] // seqs
        inner = WINDOW // shard
        fine = jax.sharding.Mesh(
            mesh.devices.reshape(heads, seqs // inner, inner), ("head", "outer", "inner")
        )
        spec = P(("outer", "inner", "head"), None)
        step = jax.shard_map(
            staged, mesh=fine, in_specs=(spec,) * 4, out_specs=(spec,) * 3, check_vma=False
        )
        return step(query, key_in, value_in, d_out)

    return run
```
